32 devices in a mesh: dp: 8 (over y, x, core), mp: 4 (over z).
Axes of the slice: x: 2, y: 2, z: 4, core: 2. Of those that a mesh axis runs over, the one named last changes fastest.
Arguments:
- tokens: bfloat16 [16384, 1024], P(('dp', 'mp')), may hold values from -6 to 6
- norm_gain: float32 [2, 1024], replicated, may hold values from 0.1 to 1.9
- qkv_weight: bfloat16 [3, 1024, 1024], P(None, 'dp', 'mp')
- out_weight: bfloat16 [1024, 1024], P('mp', 'dp'), may hold values from -0.1875 to 0.1875
- variate_bias: float32 [2, 16], replicated, may hold values from -6 to 6
- ffn_weight: bfloat16 [2, 1024, 2816], P(None, 'dp', 'mp'), may hold values from -0.1875 to 0.1875
- down_weight: bfloat16 [2816, 1024], P('mp', 'dp'), may hold values from -0.109375 to 0.109375
- sample_ids: int32 [16384], P(('dp', 'mp')), may hold values from 0 to 127, as said below
- variate_ids: int32 [16384], P(('dp', 'mp')), may hold values from 0 to 15, as said below
- time_ids: int32 [16384], P(('dp', 'mp')), may hold values from 0 to 31, as said below
Outputs:
- encoded: bfloat16 [16384, 1024], P(('dp', 'mp'))
The draws below stay inside these ranges and needn't reach their ends.
Inputs may be any that keep to these rules, and one draw needn't show every extreme that they name: `sample_ids`: within each packed sequence of 512 tokens the series numbers start at 0 and never fall; a series with v variates (1 to 16) and p patches (4 to 32) holds v * p consecutive tokens, the last series of a sequence may be cut short; some packed sequence holds 128 series of one variate and four patches each. `variate_ids`: A token's offset within its series divided by that series' patch count p. `time_ids`: A token's offset within its series modulo that series' patch count p.
All inputs are finite; a program needn't handle non-finite values.
Results may differ from the reference program's by a relative error of at most 0.017.
Values may be sent and summed in bfloat16 or wider, within the bound.
No kernel may reach another device: no remote copies, remote signals or barrier semaphores. Data moves between devices by JAX's collectives and lax.ppermute only.
A program may use at most 128 MiB of HBM per device.

```python
import jax
import jax.numpy as jnp
from jax import lax

D = 1024
HEAD_DIM = 64
HEADS = 16
FF = 2816
L = 512
SEQS = 32
TOKENS = 16384


def packing(key):
    key_var, key_pat, key_pick = jax.random.split(jax.random.fold_in(key, 5), 3)
    slots = L // 4
    variates = jax.random.randint(key_var, (SEQS, slots), 1, 17)
    patches = jax.random.randint(key_pat, (SEQS, slots), 4, 33)
    chosen = jax.random.randint(key_pick, (), 0, SEQS)
    dense = (jnp.arange(SEQS, dtype=jnp.int32) == chosen)[:, None]
    variates = jnp.where(dense, 1, variates)
    patches = jnp.where(dense, 4, patches)
    lengths = variates * patches
    ends = jnp.cumsum(lengths, axis=1)
    starts = ends - lengths
    position = jnp.arange(L, dtype=jnp.int32)
    series = jnp.sum((position[None, :, None] >= ends[:, None, :]).astype(jnp.int32), axis=2)
    begin = jnp.take_along_axis(starts, series, axis=1)
    span = jnp.take_along_axis(patches, series, axis=1)
    offset = position[None, :] - begin
    return (series.reshape(-1).astype(jnp.int32), (offset // span).reshape(-1).astype(jnp.int32), (offset % span).reshape(-1).astype(jnp.int32))


def draw_sample_ids(key, part):
    return packing(key)[0]


def draw_variate_ids(key, part):
    return packing(key)[1]


def draw_time_ids(key, part):
    return packing(key)[2]


def draw_qkv_weight(key, part):
    key_base = jax.random.fold_in(jax.random.fold_in(key, 11), 0)
    base = jax.random.normal(key_base, (3, D, D), jnp.float32) * D ** (-0.5)
    return base.astype(jnp.bfloat16)


def shard_levels(stream_key, extent, shards, least, top_value):
    level, own = 1.0, jax.random.fold_in(stream_key, 6)
    for dim, shards_of in shards:
        heights = jnp.exp(jax.random.uniform(jax.random.fold_in(own, dim), (shards_of,), jnp.float32, least / len(shards), top_value / len(shards)))
        level = level * jnp.repeat(heights, extent[dim] // shards_of).reshape([-1 if axis == dim else 1 for axis in range(len(extent))])
    return level


def gaussian(stream_key, dims, spread, most, pieces=(), held_as=jnp.bfloat16):
    level = shard_levels(stream_key, dims, pieces, -0.22, 0.18) if pieces else 1.0
    entries = jax.random.normal(stream_key, dims, jnp.float32) * spread * level
    return jnp.minimum(jnp.maximum(entries, -most), most).astype(held_as)


def setup_inputs(seed: int = 0) -> dict:
    keys = jax.random.split(jax.random.key(seed), 11)
    tokens = gaussian(keys[0], (TOKENS, D), 1.0, 6.0, ((0, 32),))
    norm_gain = jnp.clip(1.0 + 0.18 * jax.random.normal(keys[1], (2, D), jnp.float32), 0.1, 1.9)
    qkv_weight = draw_qkv_weight(jax.random.fold_in(keys[10], 71), 0)
    out_weight = gaussian(keys[3], (D, D), D ** -0.5, 0.1875, ((0, 4), (1, 8)))
    variate_bias = gaussian(keys[4], (2, HEADS), 1.5, 6.0, (), jnp.float32)
    ffn_weight = gaussian(keys[5], (2, D, FF), D ** -0.5, 0.1875, ((1, 8), (2, 4)))
    down_weight = gaussian(keys[6], (FF, D), FF ** -0.5, 0.109375, ((0, 4), (1, 8)))
    sample_ids = draw_sample_ids(jax.random.fold_in(keys[10], 71), 0)
    variate_ids = draw_variate_ids(jax.random.fold_in(keys[10], 71), 0)
    time_ids = draw_time_ids(jax.random.fold_in(keys[10], 71), 0)
    return dict(tokens=tokens, norm_gain=norm_gain, qkv_weight=qkv_weight, out_weight=out_weight, variate_bias=variate_bias, ffn_weight=ffn_weight, down_weight=down_weight, sample_ids=sample_ids, variate_ids=variate_ids, time_ids=time_ids)


def rms_norm(values, gain):
    wide = values.astype(jnp.float32)
    square = lax.optimization_barrier(jnp.mean(wide * wide, axis=-1, keepdims=True))
    return (wide * lax.rsqrt(square + 1e-05) * gain[None, :]).astype(jnp.bfloat16)

def rotate(values, times):
    half = values.shape[-1] // 2
    freq = 10000.0 ** (-jnp.arange(half, dtype=jnp.float32) / half)
    angle = times.astype(jnp.float32)[:, None] * freq[None, :]
    cosine = jnp.cos(angle)[:, None, :]
    sine = jnp.sin(angle)[:, None, :]
    first = values[..., :half]
    second = values[..., half:]
    return jnp.concatenate([first * cosine - second * sine, first * sine + second * cosine], axis=-1)

def reference(tokens, norm_gain, qkv_weight, out_weight, variate_bias, ffn_weight, down_weight, sample_ids, variate_ids, time_ids):
    total = tokens.shape[0]
    first_normed = rms_norm(tokens, norm_gain[0])
    query_raw = jnp.dot(first_normed, qkv_weight[0], preferred_element_type=jnp.float32)
    key_raw = jnp.dot(first_normed, qkv_weight[1], preferred_element_type=jnp.float32)
    value_raw = jnp.dot(first_normed, qkv_weight[2], preferred_element_type=jnp.float32)
    queries = rotate(query_raw.reshape(total, HEADS, HEAD_DIM), time_ids).astype(jnp.bfloat16)
    keys_rot = rotate(key_raw.reshape(total, HEADS, HEAD_DIM), time_ids).astype(jnp.bfloat16)
    values = value_raw.reshape(total, HEADS, HEAD_DIM).astype(jnp.bfloat16)
    count = total // L

    def one_sequence(args):
        qs, ks, vs, samples, variates = args
        scores = jnp.einsum('qhd,khd->hqk', qs.astype(jnp.float32), ks.astype(jnp.float32)) * HEAD_DIM ** (-0.5)
        same = variates[:, None] == variates[None, :]
        scores = scores + jnp.where(same[None], variate_bias[0][:, None, None], variate_bias[1][:, None, None])
        scores = jnp.where((samples[:, None] == samples[None, :])[None], scores, -1e+30)
        top = lax.optimization_barrier(jnp.max(scores, axis=2, keepdims=True))
        expo = jnp.exp(scores - top)
        weights = (expo / lax.optimization_barrier(jnp.sum(expo, axis=2, keepdims=True))).astype(jnp.bfloat16)
        return jnp.einsum('hqk,khd->qhd', weights.astype(jnp.float32), vs.astype(jnp.float32)).astype(jnp.bfloat16)
    attended = lax.map(one_sequence, (queries.reshape(count, L, HEADS, HEAD_DIM), keys_rot.reshape(count, L, HEADS, HEAD_DIM), values.reshape(count, L, HEADS, HEAD_DIM), sample_ids.reshape(count, L), variate_ids.reshape(count, L)))
    attended = attended.reshape(total, D)
    residual = (tokens.astype(jnp.float32) + jnp.dot(attended, out_weight, preferred_element_type=jnp.float32)).astype(jnp.bfloat16)
    second_normed = rms_norm(residual, norm_gain[1])
    gate = jnp.dot(second_normed, ffn_weight[0], preferred_element_type=jnp.float32)
    up = jnp.dot(second_normed, ffn_weight[1], preferred_element_type=jnp.float32)
    hidden = (jax.nn.silu(gate) * up).astype(jnp.bfloat16)
    return (residual.astype(jnp.float32) + jnp.dot(hidden, down_weight, preferred_element_type=jnp.float32)).astype(jnp.bfloat16)
```

```python
import jax
import jax.numpy as jnp
from jax import lax
from jax.experimental import pallas as pl
from jax.experimental.pallas import tpu as pltpu
from jax.sharding import PartitionSpec as P

HEAD_DIM = 64
L = 512


def rms_norm(values, gain):
    wide = values.astype(jnp.float32)
    square = jnp.mean(wide * wide, axis=-1, keepdims=True)
    return (wide * lax.rsqrt(square + 1e-05) * gain[None, :]).astype(jnp.bfloat16)


def ring(x, n, turn):
    if n == 1:
        return x[None]
    up = [(i, (i + 1) % n) for i in range(n)]
    down = [(i, (i - 1) % n) for i in range(n)]
    slots = [x] + [None] * (n - 1)
    above = below = x
    for t in range(1, (n - 1) // 2 + 1):
        above = slots[t] = lax.ppermute(above, "mp", up)
        below = slots[n - t] = lax.ppermute(below, "mp", down)
    if n % 2 == 0:
        slots[n // 2] = lax.ppermute(below, "mp", down) if turn else lax.ppermute(above, "mp", up)
    return jnp.stack(slots)


def flip(x, bit, n):
    return lax.ppermute(x, "dp", [(i, i ^ bit) for i in range(n)])


def square(x, n, turn):
    high, low = n // 2, n // 4
    from_low = flip(x, low, n)
    from_high = flip(x, high, n)
    corner = flip(from_low, high, n) if turn else flip(from_high, low, n)
    return jnp.stack([x, from_low, from_high, corner])


def doubled(x, n):
    pieces, bit = [x], 1
    while bit < n // 4:
        pieces = pieces + [flip(piece, bit, n) for piece in pieces]
        bit *= 2
    return pieces


def gather_a(x, dp, mp):
    return doubled(square(ring(x, mp, False), dp, False), dp)


def gather_b(x, dp, mp):
    return doubled(ring(square(x, dp, True), mp, True), dp)


def qkv_kernel(parts, x_ref, cos_ref, sin_ref, *refs):
    weights, outs = refs[:parts], refs[parts:]
    cosine, sine = cos_ref[...], sin_ref[...]
    width = cosine.shape[1]
    low = lax.broadcasted_iota(jnp.int32, cosine.shape, 1) % HEAD_DIM < HEAD_DIM // 2
    for j in range(3):
        total, start = None, 0
        for ref in weights:
            w = ref[:, j]
            w = w.reshape(-1, width)
            part = jnp.dot(
                x_ref[:, start : start + w.shape[0]], w, preferred_element_type=jnp.float32
            )
            start += w.shape[0]
            total = part if total is None else total + part
        if j < 2:
            half = HEAD_DIM // 2
            partner = jnp.where(low, pltpu.roll(total, width - half, 1), pltpu.roll(total, half, 1))
            total = total * cosine + partner * sine
        total = total.astype(jnp.bfloat16)
        if j == 0:
            total = total * jnp.bfloat16(HEAD_DIM ** (-0.5))
        outs[j][...] = total


def attend_kernel(heads, bias_ref, sr, sc, vr, vc, q_ref, k_ref, v_ref, o_ref, same_ref, mask_ref):
    @pl.when(pl.program_id(1) == 0)
    def _():
        same_ref[...] = jnp.where(vr[0] == vc[0], 1.0, 0.0)
        mask_ref[...] = jnp.where(sr[0] == sc[0], 0.0, -1e30)

    for h in range(heads):
        head = pl.program_id(1) * heads + h
        first, second = bias_ref[0, head], bias_ref[1, head]
        cut = slice(h * HEAD_DIM, (h + 1) * HEAD_DIM)
        scores = lax.dot_general(
            q_ref[:, cut], k_ref[:, cut], (((1,), (1,)), ((), ())),
            preferred_element_type=jnp.float32,
        )
        scores = scores + jnp.where(same_ref[...] > 0.5, first, second) + mask_ref[...]
        expo = jnp.exp(scores - jnp.max(scores, axis=1, keepdims=True))
        norm = jnp.sum(expo, axis=1, keepdims=True)
        out = jnp.dot(expo.astype(jnp.bfloat16), v_ref[:, cut], preferred_element_type=jnp.float32)
        o_ref[:, cut] = (out / norm).astype(jnp.bfloat16)


def gate_kernel(parts, x_ref, *refs):
    out_ref = refs[-1]
    results = []
    for j in range(2):
        total, start = None, 0
        for ref in refs[:parts]:
            w = ref[:, j].reshape(-1, ref.shape[-1])
            part = jnp.dot(
                x_ref[:, start : start + w.shape[0]], w, preferred_element_type=jnp.float32
            )
            start += w.shape[0]
            total = part if total is None else total + part
        results.append(total)
    gate, up = results
    out_ref[...] = (gate / (1.0 + jnp.exp(-gate)) * up).astype(jnp.bfloat16)


def rows_kernel(parts, groups, cuts, place, *refs):
    order_ref, x_ref, base_ref = refs[1:4]
    weights, out_ref = refs[4:-1], refs[-1]
    for p in range(parts):

        @pl.when(pl.program_id(0) // 4 == p)
        def _(p=p):
            total = base_ref[...].astype(jnp.float32)
            for g in range(groups):
                ref = weights[g * parts + p]
                for t in range(x_ref.shape[0]):
                    total += jnp.dot(
                        x_ref[order_ref[t], :, cuts[g] : cuts[g + 1]], ref[t],
                        preferred_element_type=jnp.float32,
                    )
            out_ref[...] = total.astype(jnp.bfloat16)


def local(
    tokens, norm_gain, qkv_weight, out_weight, variate_bias, ffn_weight, down_weight,
    sample_ids, variate_ids, time_ids,
):
    dp, mp = lax.axis_size("dp"), lax.axis_size("mp")
    me, slab = lax.axis_index("dp"), lax.axis_index("mp")
    rows, width = tokens.shape
    parts = dp // 4
    part_rows, part_cols = qkv_weight.shape[1:]
    hidden_cols = ffn_weight.shape[2]
    block = out_weight.shape[1]
    limit = 60 * 1024 * 1024

    slot = jnp.arange(dp, dtype=jnp.int32)
    source = me ^ (slot // 4 + (slot % 4) * (dp // 4))

    def params(*kinds):
        return pltpu.CompilerParams(vmem_limit_bytes=limit, dimension_semantics=kinds)

    def all_devices(x):
        return lax.all_gather(x, ("dp", "mp")).reshape((dp, mp) + x.shape)

    qkv_full = all_devices(qkv_weight)
    ffn_full = all_devices(ffn_weight)
    out_b = gather_b(out_weight, dp, mp)
    down_a = gather_a(down_weight, dp, mp)

    x = rms_norm(tokens, norm_gain[0])
    half = HEAD_DIM // 2
    freq = 10000.0 ** (-jnp.arange(half, dtype=jnp.float32) / half)
    angle = time_ids.astype(jnp.float32)[:, None] * freq[None, :]
    heads_slab = part_cols // HEAD_DIM
    cosine = jnp.tile(jnp.cos(angle), (1, 2 * heads_slab))
    sine = jnp.sin(angle)
    sine = jnp.tile(jnp.concatenate([-sine, sine], axis=1), (1, heads_slab))
    whole = lambda shape: pl.BlockSpec(shape, lambda *_: (0,) * len(shape))
    spec_a = pl.BlockSpec((dp, None, 3, part_rows, part_cols), lambda t: (0, t, 0, 0, 0))
    slab_spec = pl.BlockSpec((rows, part_cols), lambda t: (0, t))
    queries, keys, values = pl.pallas_call(
        lambda *refs: qkv_kernel(1, *refs),
        grid=(mp,),
        in_specs=[whole((rows, width)), whole(cosine.shape), whole(sine.shape)]
        + [spec_a],
        out_specs=[slab_spec] * 3,
        out_shape=[jax.ShapeDtypeStruct((rows, width), jnp.bfloat16)] * 3,
        compiler_params=params("arbitrary"),
        name="qkv",
    )(x, cosine, sine, qkv_full)

    order = (slab - jnp.arange(mp, dtype=jnp.int32)) % mp
    count = rows // L
    pair = 2
    row_ids = pl.BlockSpec((1, L, 1), lambda s, h: (s, 0, 0))
    col_ids = pl.BlockSpec((1, 1, L), lambda s, h: (s, 0, 0))
    head_spec = pl.BlockSpec((L, pair * HEAD_DIM), lambda s, h: (s, h))
    attended = pl.pallas_call(
        lambda *refs: attend_kernel(pair, *refs),
        grid=(count, width // (pair * HEAD_DIM)),
        in_specs=[pl.BlockSpec(memory_space=pltpu.SMEM), row_ids, col_ids, row_ids, col_ids]
        + [head_spec] * 3,
        out_specs=head_spec,
        out_shape=jax.ShapeDtypeStruct((rows, width), jnp.bfloat16),
        scratch_shapes=[pltpu.VMEM((L, L), jnp.float32)] * 2,
        compiler_params=params("arbitrary", "arbitrary"),
        name="attend",
    )(
        variate_bias,
        sample_ids.reshape(count, L, 1), sample_ids.reshape(count, 1, L),
        variate_ids.reshape(count, L, 1), variate_ids.reshape(count, 1, L),
        queries, keys, values,
    )

    place = block % 128 == 0

    def row_parallel(x, base, groups, name):
        cuts, specs, operands = [0], [], []
        for pieces, layout, size in groups:
            cuts.append(cuts[-1] + size)
            for p in range(parts):
                if layout == "a":
                    shape = (None, mp, size, block)
                    index = lambda e, src, _, p=p: (jnp.where(e // 4 == p, e % 4, jnp.where(e // 4 < p, 0, 3)), 0, 0, 0)
                else:
                    shape = (mp, None, size, block)
                    index = lambda e, src, _, p=p: (0, jnp.where(e // 4 == p, e % 4, jnp.where(e // 4 < p, 0, 3)), 0, 0)
                specs.append(pl.BlockSpec(shape, index))
            operands += pieces
        if place:
            tile = pl.BlockSpec((rows, block), lambda e, src, _: (0, src[e]))
            shape = (rows, width)
        else:
            tile = pl.BlockSpec((None, rows, block), lambda e, src, _: (src[e], 0, 0))
            shape = (dp, rows, block)
            base = base.reshape(rows, dp, block).swapaxes(0, 1)
        result = pl.pallas_call(
            lambda *refs: rows_kernel(parts, len(groups), cuts, place, *refs),
            grid_spec=pltpu.PrefetchScalarGridSpec(
                num_scalar_prefetch=2,
                grid=(dp,),
                in_specs=[pl.BlockSpec(x.shape, lambda e, src, _: (0, 0, 0)), tile] + specs,
                out_specs=tile,
            ),
            out_shape=jax.ShapeDtypeStruct(shape, jnp.bfloat16),
            compiler_params=params("arbitrary"),
            name=name,
        )(source, order, x, base, *operands)
        return result if place else result.swapaxes(0, 1).reshape(rows, width)

    residual = row_parallel(
        attended.reshape(rows, mp, part_cols).swapaxes(0, 1), tokens,
        [(out_b, "b", part_cols)], "mix",
    )
    second_normed = rms_norm(residual, norm_gain[1])
    hidden = pl.pallas_call(
        lambda *refs: gate_kernel(1, *refs),
        grid=(mp,),
        in_specs=[whole((rows, width))]
        + [pl.BlockSpec((dp, None, 2, part_rows, hidden_cols), lambda t: (0, t, 0, 0, 0))],
        out_specs=pl.BlockSpec((None, rows, hidden_cols), lambda t: (t, 0, 0)),
        out_shape=jax.ShapeDtypeStruct((mp, rows, hidden_cols), jnp.bfloat16),
        compiler_params=params("arbitrary"),
        name="gate",
    )(second_normed, ffn_full)
    return row_parallel(hidden, residual, [(down_a, "a", hidden_cols)], "down")


def solution(mesh):
    return jax.shard_map(
        local,
        mesh=mesh,
        in_specs=(
            P(("dp", "mp"), None),
            P(),
            P(None, "dp", "mp"),
            P("mp", "dp"),
            P(),
            P(None, "dp", "mp"),
            P("mp", "dp"),
            P(("dp", "mp")),
            P(("dp", "mp")),
            P(("dp", "mp")),
        ),
        out_specs=P(("dp", "mp"), None),
        check_vma=False,
    )
```
